32 devices in a mesh: groups: 2 (over x), seq: 4 (over y, core), head: 4 (over z).
Axes of the slice: x: 2, y: 2, z: 4, core: 2. Of those that a mesh axis runs over, the one named last changes fastest.
Arguments:
- query: bfloat16 [32, 16, 1024], P('groups', None, 'head'), parts along dimension 0, may hold values from -6 to 6, as said below
- new_key: bfloat16 [32, 16, 1024], P('groups', None, 'head'), parts along dimension 0, may hold values from -6 to 6
- new_value: bfloat16 [32, 16, 1024], P('groups', None, 'head'), parts along dimension 0, may hold values from -6 to 6
- keys: bfloat16 [32, 4096, 1024], P('groups', 'seq', 'head'), parts along dimension 0, may hold values from -6 to 6, as said below
- values: bfloat16 [32, 4096, 1024], P('groups', 'seq', 'head'), parts along dimension 0, may hold values from -6 to 6
- lengths: int32 [32], P('groups'), parts along dimension 0, may hold values from 2 to 4096
- time_bucket: int32 [32, 4096], P('groups', 'seq'), parts along dimension 0, may hold values from 0 to 63
- action: int32 [32, 4096], P('groups', 'seq'), parts along dimension 0, may hold values from 0 to 15
- time_bias: float32 [64, 8], P(None, 'head'), may hold values from -0.25 to 0.25
- action_bias: float32 [16, 8], P(None, 'head'), may hold values from -0.25 to 0.25
- gate: bfloat16 [32, 16, 1024], P('groups', None, 'head'), parts along dimension 0, may hold values from -6 to 6
- norm_gain: float32 [1024], P('head'), may hold values from 0.1 to 1.9
- w_out: bfloat16 [1024, 1024], P('head'), may hold values from -0.1875 to 0.1875
Outputs:
- output: bfloat16 [32, 16, 1024], P(('groups', 'seq'), None, 'head'), parts along dimension 0
The draws below stay inside these ranges and needn't reach their ends.
There are 2 independent parts, one for each index of `groups`. The reference program is written for one: setup_inputs(seed, part) draws one part's arguments, and reference() takes and returns one part's arrays. A program takes and returns all parts, laid end to end along the dimension named above; an argument that names none is the same for every part. Nothing has to cross between parts.
Inputs may be any that keep to these rules, and one draw needn't show every extreme that they name: `query`: queries of order one; some users' queries may be large and equal to some of their keys. `keys`: keys of order one.
All inputs are finite; a program needn't handle non-finite values.
Results may differ from the reference program's by a relative error of at most 0.0056.
Values sent between devices are 32-bit elements; how exact they have to be, the bound alone decides.
A program may use at most 64 MiB of HBM per device.

```python
import math
import jax
import jax.numpy as jnp
from jax import lax

USERS = 16
CANDS = 16
S_DEV = 1024
HEADS = 8
DH = 128
D_MODEL = 1024
BUCKETS = 64
ACTIONS = 16
HISTORY = 4096
N_SEQ = 4


def draw_query(key, part):
    result = jax.random.truncated_normal(jax.random.fold_in(key, 1), -6.0, 6.0, (USERS, CANDS, HEADS * DH), jnp.float32)
    return result.astype(jnp.bfloat16)


def draw_keys(key, part):
    result = jax.random.truncated_normal(jax.random.fold_in(key, 2), -6.0, 6.0, (USERS, HISTORY, HEADS * DH), jnp.float32)
    return result.astype(jnp.bfloat16)


def plant(values, key, smallest, top_value):
    place = [jax.random.randint(jax.random.fold_in(key, axis), (), 0, length) for axis, length in enumerate(values.shape)]
    widest = values.shape.index(max(values.shape))
    beside = place[:widest] + [(place[widest] + 1) % values.shape[widest]] + place[widest + 1:]
    return values.at[tuple(place)].set(smallest).at[tuple(beside)].set(top_value)


def block_levels(key, dims, split, least, largest):
    def one(dim, blocks):
        steps = jax.random.uniform(jax.random.fold_in(jax.random.fold_in(key, 6), dim), (blocks,), jnp.float32, least / len(split), largest / len(split))
        return jnp.repeat(jnp.exp(steps), dims[dim] // blocks).reshape((-1,) + (1,) * (len(dims) - dim - 1))

    gain = one(*split[0])
    for cut in split[1:]:
        gain = gain * one(*cut)
    return gain


def noise(stream_key, extent, scale, bound, split=(), held_as=jnp.bfloat16):
    values = scale * jax.random.normal(stream_key, extent, jnp.float32)
    if split:
        values = values * block_levels(stream_key, extent, split, -0.22, 0.18)
    return jnp.clip(values, -bound, bound).astype(held_as)


def setup_inputs(seed: int = 0, part: int = 0) -> dict:
    splits = jax.random.split(jax.random.key(seed), 14)
    own_keys = jax.random.split(jax.random.fold_in(splits[13], part), 14)
    return {
        "query": draw_query(jax.random.fold_in(jax.random.fold_in(splits[13], part), 71), part),
        "new_key": noise(own_keys[1], (USERS, CANDS, HEADS * DH), 1.0, 6.0, ((2, 4),)),
        "new_value": noise(own_keys[2], (USERS, CANDS, HEADS * DH), 1.0, 6.0, ((2, 4),)),
        "keys": draw_keys(jax.random.fold_in(jax.random.fold_in(splits[13], part), 71), part),
        "values": noise(own_keys[4], (USERS, HISTORY, HEADS * DH), 1.0, 6.0, ((1, 4), (2, 4))),
        "lengths": plant(jax.random.randint(own_keys[5], (USERS,), 2, HISTORY + 1), jax.random.fold_in(own_keys[5], 1), 2, HISTORY).astype(jnp.int32),
        "time_bucket": plant(jax.random.randint(own_keys[6], (USERS, HISTORY), 0, BUCKETS), jax.random.fold_in(own_keys[6], 1), 0, BUCKETS - 1).astype(jnp.int32),
        "action": plant(jax.random.randint(own_keys[7], (USERS, HISTORY), 0, ACTIONS), jax.random.fold_in(own_keys[7], 1), 0, ACTIONS - 1).astype(jnp.int32),
        "time_bias": jnp.clip(jax.random.uniform(splits[8], (BUCKETS, HEADS), jnp.float32, -0.25, 0.25) * block_levels(splits[8], (BUCKETS, HEADS), ((1, 4),), -0.4, 0.0), -0.25, 0.25),
        "action_bias": jnp.clip(jax.random.uniform(splits[9], (ACTIONS, HEADS), jnp.float32, -0.25, 0.25) * block_levels(splits[9], (ACTIONS, HEADS), ((1, 4),), -0.4, 0.0), -0.25, 0.25),
        "gate": noise(own_keys[10], (USERS, CANDS, HEADS * DH), 1.0, 6.0, ((2, 4),)),
        "norm_gain": jnp.clip(1.0 + 0.18 * jax.random.normal(splits[11], (HEADS * DH,), jnp.float32), 0.1, 1.9),
        "w_out": noise(splits[12], (HEADS * DH, D_MODEL), (HEADS * DH) ** -0.5, 0.1875, ((0, 4),)),
    }


def reference(query, new_key, new_value, keys, values, lengths, time_bucket, action, time_bias, action_bias, gate, norm_gain, w_out):
    user_count = keys.shape[0]
    cand_count = query.shape[1]
    head_count = HEADS
    head_size = DH
    score_scale = 1.0 / math.sqrt(head_size)
    query_heads = query.astype(jnp.float32).reshape(user_count, cand_count, head_count, head_size)

    def one_block(block_index):
        first = (block_index * S_DEV).astype(jnp.int32)
        key_block = lax.dynamic_slice_in_dim(keys, first, S_DEV, 1).astype(jnp.float32).reshape(user_count, S_DEV, head_count, head_size)
        value_block = lax.dynamic_slice_in_dim(values, first, S_DEV, 1).astype(jnp.float32).reshape(user_count, S_DEV, head_count, head_size)
        bucket_block = lax.dynamic_slice_in_dim(time_bucket, first, S_DEV, 1)
        action_block = lax.dynamic_slice_in_dim(action, first, S_DEV, 1)
        scores = jnp.einsum('uchd,ushd->uchs', query_heads, key_block) * score_scale
        biases = jnp.transpose(time_bias[bucket_block], (0, 2, 1)) + jnp.transpose(action_bias[action_block], (0, 2, 1))
        scores = scores + biases[:, None]
        position = first + jnp.arange(S_DEV, dtype=jnp.int32)
        valid = position[None, None, None, :] < lengths[:, None, None, None]
        block_max = lax.optimization_barrier(jnp.max(jnp.where(valid, scores, -1e+30), axis=-1))
        weights = jnp.where(valid, jnp.exp(scores - block_max[..., None]), 0.0)
        block_sum = lax.optimization_barrier(jnp.sum(weights, axis=-1))
        rounded = weights.astype(jnp.bfloat16).astype(jnp.float32)
        block_acc = jnp.einsum('uchs,ushd->uchd', rounded, value_block)
        return (block_max, block_sum, block_acc)
    maxima, sums, accs = lax.map(one_block, jnp.arange(N_SEQ, dtype=jnp.int32))
    own = lax.optimization_barrier(jnp.sum(query_heads * new_key.astype(jnp.float32).reshape(user_count, cand_count, head_count, head_size), axis=-1)) * score_scale
    overall = jnp.maximum(lax.optimization_barrier(jnp.max(maxima, axis=0)), own)
    factors = jnp.exp(maxima - overall[None])
    own_factor = jnp.exp(own - overall)
    numer = lax.optimization_barrier(jnp.sum(factors[..., None] * accs, axis=0)) + own_factor[..., None] * new_value.astype(jnp.float32).reshape(user_count, cand_count, head_count, head_size)
    denom = lax.optimization_barrier(jnp.sum(factors * sums, axis=0)) + own_factor
    attended = numer / denom[..., None]
    square_sum = lax.optimization_barrier(jnp.sum(jnp.square(attended), axis=(2, 3)))
    gate_heads = gate.astype(jnp.float32).reshape(user_count, cand_count, head_count, head_size)
    hidden = (attended * norm_gain.reshape(head_count, head_size) * jax.nn.silu(gate_heads)).astype(jnp.bfloat16)
    hidden = hidden.reshape(user_count * cand_count, head_count * head_size)
    projected = jnp.dot(hidden, w_out, preferred_element_type=jnp.float32).reshape(user_count, cand_count, -1)
    factor = 1.0 / jnp.sqrt(square_sum / (head_count * head_size) + 1e-06)
    return (projected * factor[:, :, None]).astype(jnp.bfloat16)
```

```python
import functools
import math

import jax
import jax.numpy as jnp
from jax import lax
from jax.experimental import pallas as pl
from jax.experimental.pallas import tpu as pltpu
from jax.sharding import PartitionSpec as P

MESH = pl.DeviceIdType.MESH
LANES = 128
LOG2E = math.log2(math.e)
INVALID = -1e30
FLOOR = -1e29
NT = (((1,), (1,)), ((), ()))


def partner(rank, step, count):
    result, bit = 0, 1
    while bit < count:
        held = (rank // bit) % 2
        result = result + bit * (1 - held if (step // bit) % 2 else held)
        bit *= 2
    return result


def column_to_row(column, first, lanes):
    shape = (column.shape[0], lanes)
    row_id = lax.broadcasted_iota(jnp.int32, shape, 0)
    lane_id = lax.broadcasted_iota(jnp.int32, shape, 1)
    return jnp.sum(jnp.where(lane_id == row_id + first, column, 0.0), axis=0, keepdims=True)


def row_to_column(row, first, count):
    shape = (count, row.shape[1])
    row_id = lax.broadcasted_iota(jnp.int32, shape, 0)
    lane_id = lax.broadcasted_iota(jnp.int32, shape, 1)
    return jnp.sum(jnp.where(lane_id == row_id + first, row, 0.0), axis=1, keepdims=True)


def kernel(
    dims,
    len_ref,
    q_hbm,
    nk_hbm,
    nv_hbm,
    k_hbm,
    v_hbm,
    bucket_hbm,
    action_hbm,
    tb_hbm,
    ab_hbm,
    gate_hbm,
    gain_hbm,
    w_hbm,
    out_ref,
    q_s,
    nk_s,
    nv_s,
    k_s,
    v_s,
    bucket_s,
    action_s,
    tb_s,
    ab_s,
    gate_s,
    gain_s,
    w_s,
    bias_s,
    part_s,
    got_s,
    zpart_s,
    zgot_s,
    k_sem,
    v_sem,
    in_sem,
    late_sem,
    send_sem,
    recv_sem,
    zsend_sem,
    zrecv_sem,
):
    users, cands, block, heads, size, seqs, slices, local, out_cols = dims
    rows = heads * cands
    width = heads * size
    me = lax.axis_index("seq")
    mh = lax.axis_index("head")
    scale = LOG2E / math.sqrt(size)

    barrier = pltpu.get_barrier_semaphore()
    for step in range(1, seqs):
        pl.semaphore_signal(
            barrier, inc=1, device_id={"seq": partner(me, step, seqs)}, device_id_type=MESH
        )
    for step in range(1, slices):
        pl.semaphore_signal(
            barrier, inc=1, device_id={"head": (mh + step) % slices}, device_id_type=MESH
        )

    early = [
        pltpu.make_async_copy(source, target, in_sem.at[i])
        for i, (source, target) in enumerate(
            (
                (tb_hbm, tb_s),
                (ab_hbm, ab_s),
                (bucket_hbm, bucket_s),
                (action_hbm, action_s),
                (q_hbm, q_s),
            )
        )
    ]
    mine = pl.ds(me * local, local)
    late = [
        pltpu.make_async_copy(source, target, late_sem.at[i])
        for i, (source, target) in enumerate(
            (
                (nk_hbm.at[mine], nk_s),
                (nv_hbm.at[mine], nv_s),
                (gate_hbm.at[mine], gate_s),
                (gain_hbm, gain_s),
                (w_hbm, w_s),
            )
        )
    ]
    for copy in early:
        copy.start()
    order = []
    for turn in range(local):
        for step in range(seqs - 1, -1, -1):
            slot = len(order)
            user = partner(me, step, seqs) * local + turn
            k_copy = pltpu.make_async_copy(k_hbm.at[user], k_s.at[slot], k_sem.at[slot])
            v_copy = pltpu.make_async_copy(v_hbm.at[user], v_s.at[slot], v_sem.at[slot])
            k_copy.start()
            v_copy.start()
            order.append((turn, step, user, k_copy, v_copy))
        if turn == 0:
            for copy in late:
                copy.start()

    for copy in early:
        copy.wait()

    def table(ref, head):
        count = ref.shape[0]
        return column_to_row(ref[:, head : head + 1] * LOG2E, 0, LANES)

    for head in range(heads):
        tb_row = jnp.broadcast_to(table(tb_s, head), (users, LANES))
        ab_row = jnp.broadcast_to(table(ab_s, head), (users, LANES))
        for chunk in range(block // LANES):
            lanes = slice(chunk * LANES, (chunk + 1) * LANES)
            bias_s[head, :, lanes] = jnp.take_along_axis(
                tb_row, bucket_s[:, lanes], axis=1
            ) + jnp.take_along_axis(ab_row, action_s[:, lanes], axis=1)

    position = me * block + lax.broadcasted_iota(jnp.int32, (1, block), 1)
    lane_of = lax.broadcasted_iota(jnp.int32, (cands, width), 1)

    def split_query(query):
        return jnp.concatenate(
            [
                jnp.where(lane_of // size == head, query, jnp.zeros_like(query))
                for head in range(heads)
            ],
            axis=0,
        )

    def attend(slot):
        turn, step, user, _, _ = order[slot]
        raw = lax.dot_general(
            split_query(q_s[user]), k_s[slot], NT, preferred_element_type=jnp.float32
        )
        valid = position < len_ref[user]
        bias = jnp.concatenate(
            [
                jnp.broadcast_to(
                    jnp.where(valid, bias_s[head, pl.ds(user, 1), :], INVALID), (cands, block)
                )
                for head in range(heads)
            ],
            axis=0,
        )
        scores = raw * scale + bias
        top = jnp.maximum(jnp.max(scores, axis=1, keepdims=True), FLOOR)
        weights = jnp.exp2(scores - top)
        total = jnp.sum(weights, axis=1, keepdims=True)
        mixed = jnp.dot(
            weights.astype(jnp.bfloat16), v_s[slot], preferred_element_type=jnp.float32
        )
        for head in range(heads):
            held = slice(head * cands, (head + 1) * cands)
            part_s[turn, step, held, :] = mixed[held, head * size : (head + 1) * size]
        stats = column_to_row(top, 0, size) + column_to_row(total, rows, size)
        part_s[turn, step, rows : rows + 8, :] = jnp.broadcast_to(stats, (8, size))

    def exchange(turn, step):
        return pltpu.make_async_remote_copy(
            src_ref=part_s.at[turn, step],
            dst_ref=got_s.at[turn, step - 1],
            send_sem=send_sem.at[turn, step - 1],
            recv_sem=recv_sem.at[turn, step - 1],
            device_id={"seq": partner(me, step, seqs)},
            device_id_type=MESH,
        )

    def spread(turn, step):
        target = (mh + step) % slices
        return pltpu.make_async_remote_copy(
            src_ref=zpart_s.at[turn, target],
            dst_ref=zgot_s.at[turn, step - 1],
            send_sem=zsend_sem.at[turn, step - 1],
            recv_sem=zrecv_sem.at[turn, step - 1],
            device_id={"head": target},
            device_id_type=MESH,
        )

    def combine(turn):
        for step in range(1, seqs):
            exchange(turn, step).wait_recv()
        blocks = [part_s.at[turn, 0]] + [got_s.at[turn, step - 1] for step in range(1, seqs)]
        query = q_s[me * local + turn].astype(jnp.float32)
        new_key = nk_s[turn].astype(jnp.float32)
        new_value = nv_s[turn].astype(jnp.float32)
        product = query * new_key

        def by_head(source):
            return jnp.concatenate(
                [source[:, head * size : (head + 1) * size] for head in range(heads)], axis=0
            )

        own = jnp.sum(by_head(product), axis=1, keepdims=True) * scale
        maxima = [row_to_column(ref[rows : rows + 1, :], 0, rows) for ref in blocks]
        sums = [row_to_column(ref[rows : rows + 1, :], rows, rows) for ref in blocks]
        top = functools.reduce(jnp.maximum, maxima, own)
        own_factor = jnp.exp2(own - top)
        numer = own_factor * by_head(new_value)
        denom = own_factor
        for ref, high, amount in zip(blocks, maxima, sums):
            factor = jnp.exp2(high - top)
            numer = numer + factor * ref[:rows, :]
            denom = denom + factor * amount
        attended = numer / denom
        squares = jnp.sum(jnp.square(attended), axis=1, keepdims=True)
        square = squares[:cands]
        for head in range(1, heads):
            square = square + squares[head * cands : (head + 1) * cands]
        wide = jnp.concatenate(
            [attended[head * cands : (head + 1) * cands] for head in range(heads)], axis=1
        )
        gate = gate_s[turn].astype(jnp.float32)
        gain = gain_s[...].reshape(1, width)
        hidden = (wide * gain * (gate / (1.0 + jnp.exp(-gate)))).astype(jnp.bfloat16)
        projected = jnp.dot(hidden, w_s[...], preferred_element_type=jnp.float32)
        square_row = jnp.broadcast_to(column_to_row(square, 0, out_cols), (8, out_cols))
        for target in range(slices):
            zpart_s[turn, target, :cands, :] = projected[
                :, target * out_cols : (target + 1) * out_cols
            ]
            zpart_s[turn, target, cands : cands + 8, :] = square_row
        for step in range(1, slices):
            spread(turn, step).start()

    def finish(turn):
        total = zpart_s[turn, mh]
        for step in range(1, slices):
            spread(turn, step).wait_recv()
            total = total + zgot_s[turn, step - 1]
        square = row_to_column(total[cands : cands + 1, :], 0, cands)
        factor = 1.0 / jnp.sqrt(square / (width * slices) + 1e-6)
        out_ref[turn] = (total[:cands] * factor).astype(out_ref.dtype)

    for turn in range(local):
        for step in range(seqs - 1, -1, -2):
            slots = [turn * seqs + seqs - 1 - step]
            if step:
                slots.append(slots[0] + 1)
            for slot in slots:
                order[slot][3].wait()
                order[slot][4].wait()
            for slot in slots:
                attend(slot)
            if turn == 0 and step == seqs - 1:
                pl.semaphore_wait(barrier, seqs - 1 + slices - 1)
            for slot in slots:
                if order[slot][1]:
                    exchange(turn, order[slot][1]).start()
        if turn == 0:
            for copy in late:
                copy.wait()
        else:
            combine(turn - 1)
    combine(local - 1)
    for turn in range(local):
        finish(turn)
    for turn in range(local):
        for step in range(1, seqs):
            exchange(turn, step).wait_send()
        for step in range(1, slices):
            spread(turn, step).wait_send()


def body(
    query,
    new_key,
    new_value,
    keys,
    values,
    lengths,
    time_bucket,
    action,
    time_bias,
    action_bias,
    gate,
    norm_gain,
    w_out,
):
    users, block, width = keys.shape
    cands = query.shape[1]
    heads = time_bias.shape[1]
    size = width // heads
    seqs = lax.axis_size("seq")
    slices = lax.axis_size("head")
    local = users // seqs
    rows = heads * cands
    out_cols = w_out.shape[1] // slices
    dims = (users, cands, block, heads, size, seqs, slices, local, out_cols)
    f32, bf16 = jnp.float32, jnp.bfloat16
    anywhere = pl.BlockSpec(memory_space=pl.ANY)
    return pl.pallas_call(
        functools.partial(kernel, dims),
        out_shape=jax.ShapeDtypeStruct((local, cands, out_cols), bf16),
        in_specs=[pl.BlockSpec(memory_space=pltpu.SMEM)] + [anywhere] * 12,
        out_specs=pl.BlockSpec(memory_space=pltpu.VMEM),
        scratch_shapes=[
            pltpu.VMEM((users, cands, width), bf16),
            pltpu.VMEM((local, cands, width), bf16),
            pltpu.VMEM((local, cands, width), bf16),
            pltpu.VMEM((users, block, width), bf16),
            pltpu.VMEM((users, block, width), bf16),
            pltpu.VMEM((users, block), jnp.int32),
            pltpu.VMEM((users, block), jnp.int32),
            pltpu.VMEM(time_bias.shape, f32),
            pltpu.VMEM(action_bias.shape, f32),
            pltpu.VMEM((local, cands, width), bf16),
            pltpu.VMEM((width,), f32),
            pltpu.VMEM(w_out.shape, bf16),
            pltpu.VMEM((heads, users, block), f32),
            pltpu.VMEM((local, seqs, rows + 8, size), f32),
            pltpu.VMEM((local, seqs - 1, rows + 8, size), f32),
            pltpu.VMEM((local, slices, cands + 8, out_cols), f32),
            pltpu.VMEM((local, slices - 1, cands + 8, out_cols), f32),
            pltpu.SemaphoreType.DMA((users,)),
            pltpu.SemaphoreType.DMA((users,)),
            pltpu.SemaphoreType.DMA((5,)),
            pltpu.SemaphoreType.DMA((5,)),
            pltpu.SemaphoreType.DMA((local, seqs - 1)),
            pltpu.SemaphoreType.DMA((local, seqs - 1)),
            pltpu.SemaphoreType.DMA((local, slices - 1)),
            pltpu.SemaphoreType.DMA((local, slices - 1)),
        ],
        compiler_params=pltpu.CompilerParams(
            collective_id=0, has_side_effects=True, vmem_limit_bytes=48 * 1024 * 1024
        ),
    )(
        lengths,
        query,
        new_key,
        new_value,
        keys,
        values,
        time_bucket,
        action,
        time_bias,
        action_bias,
        gate,
        norm_gain,
        w_out,
    )


def solution(mesh):
    placed = (
        P("groups", None, "head"),
        P("groups", None, "head"),
        P("groups", None, "head"),
        P("groups", "seq", "head"),
        P("groups", "seq", "head"),
        P("groups"),
        P("groups", "seq"),
        P("groups", "seq"),
        P(None, "head"),
        P(None, "head"),
        P("groups", None, "head"),
        P("head"),
        P("head", None),
    )
    return jax.shard_map(
        body,
        mesh=mesh,
        in_specs=placed,
        out_specs=P(("groups", "seq"), None, "head"),
        check_vma=False,
    )
```

```python
import functools
import math

import jax
import jax.numpy as jnp
from jax import lax
from jax.experimental import pallas as pl
from jax.experimental.pallas import tpu as pltpu
from jax.sharding import PartitionSpec as P

MESH = pl.DeviceIdType.MESH
LANES = 128
LOG2E = math.log2(math.e)
AHEAD = 4
INVALID = -1e30
FLOOR = -1e29
NT = (((1,), (1,)), ((), ()))


def partner(rank, step, count):
    result, bit = 0, 1
    while bit < count:
        held = (rank // bit) % 2
        result = result + bit * (1 - held if (step // bit) % 2 else held)
        bit *= 2
    return result


def column_to_row(column, first, lanes):
    shape = (column.shape[0], lanes)
    row_id = lax.broadcasted_iota(jnp.int32, shape, 0)
    lane_id = lax.broadcasted_iota(jnp.int32, shape, 1)
    return jnp.sum(jnp.where(lane_id == row_id + first, column, 0.0), axis=0, keepdims=True)


def row_to_column(row, first, count):
    shape = (count, row.shape[1])
    row_id = lax.broadcasted_iota(jnp.int32, shape, 0)
    lane_id = lax.broadcasted_iota(jnp.int32, shape, 1)
    return jnp.sum(jnp.where(lane_id == row_id + first, row, 0.0), axis=1, keepdims=True)


def kernel(
    dims,
    len_hbm,
    q_hbm,
    nk_hbm,
    nv_hbm,
    k_hbm,
    v_hbm,
    bucket_hbm,
    action_hbm,
    tb_hbm,
    ab_hbm,
    gate_hbm,
    gain_hbm,
    w_hbm,
    out_ref,
    len_ref,
    q_s,
    nk_s,
    nv_s,
    k_s,
    v_s,
    bucket_s,
    action_s,
    tb_s,
    ab_s,
    gate_s,
    gain_s,
    w_s,
    bias_s,
    part_s,
    got_s,
    zpart_s,
    zgot_s,
    square_s,
    squares_s,
    k_sem,
    v_sem,
    in_sem,
    late_sem,
    send_sem,
    recv_sem,
    zsend_sem,
    zrecv_sem,
    tsend_sem,
    trecv_sem,
):
    users, cands, block, heads, size, seqs, slices, local, out_cols = dims
    rows = heads * cands
    width = heads * size
    me = lax.axis_index("seq")
    mh = lax.axis_index("head")
    scale = LOG2E / math.sqrt(size)

    barrier = pltpu.get_barrier_semaphore()
    for step in range(1, seqs):
        pl.semaphore_signal(
            barrier, inc=1, device_id={"seq": partner(me, step, seqs)}, device_id_type=MESH
        )
    for step in range(1, slices):
        pl.semaphore_signal(
            barrier, inc=1, device_id={"head": (mh + step) % slices}, device_id_type=MESH
        )

    early = [
        pltpu.make_async_copy(source, target, in_sem.at[i])
        for i, (source, target) in enumerate(
            (
                (len_hbm, len_ref),
                (tb_hbm, tb_s),
                (ab_hbm, ab_s),
                (bucket_hbm, bucket_s),
                (action_hbm, action_s),
                (q_hbm, q_s),
            )
        )
    ]
    mine = pl.ds(me * local, local)
    late = [
        pltpu.make_async_copy(source, target, late_sem.at[i])
        for i, (source, target) in enumerate(
            (
                (nk_hbm.at[mine], nk_s),
                (nv_hbm.at[mine], nv_s),
                (gate_hbm.at[mine], gate_s),
                (gain_hbm, gain_s),
                (w_hbm, w_s),
            )
        )
    ]
    for copy in early:
        copy.start()
    order = []
    for turn in range(local):
        for step in range(seqs - 1, -1, -1):
            slot = len(order)
            user = partner(me, step, seqs) * local + turn
            k_copy = pltpu.make_async_copy(k_hbm.at[user], k_s.at[slot], k_sem.at[slot])
            v_copy = pltpu.make_async_copy(v_hbm.at[user], v_s.at[slot], v_sem.at[slot])
            order.append((turn, step, user, k_copy, v_copy))

    def fetch(slot):
        if slot < users:
            order[slot][3].start()
            order[slot][4].start()

    for slot in range(AHEAD):
        fetch(slot)

    square_s[...] = jnp.zeros_like(square_s)
    for copy in early:
        copy.wait()

    def table(ref, head):
        row = ref[head : head + 1, :] * LOG2E
        return jnp.concatenate([row, jnp.zeros((1, LANES - row.shape[1]), row.dtype)], axis=1)

    for head in range(heads):
        tb_row = jnp.broadcast_to(table(tb_s, head), (users, LANES))
        ab_row = jnp.broadcast_to(table(ab_s, head), (users, LANES))
        for chunk in range(block // LANES):
            lanes = slice(chunk * LANES, (chunk + 1) * LANES)
            bias_s[head, :, lanes] = jnp.take_along_axis(
                tb_row, bucket_s[:, lanes], axis=1
            ) + jnp.take_along_axis(ab_row, action_s[:, lanes], axis=1)

    position = me * block + lax.broadcasted_iota(jnp.int32, (1, block), 1)
    lane_of = lax.broadcasted_iota(jnp.int32, (cands, width), 1)

    def split_query(query):
        return jnp.concatenate(
            [
                jnp.where(lane_of // size == head, query, jnp.zeros_like(query))
                for head in range(heads)
            ],
            axis=0,
        )

    def attend(slot):
        turn, step, user, _, _ = order[slot]
        raw = lax.dot_general(
            split_query(q_s[user]), k_s[slot], NT, preferred_element_type=jnp.float32
        )
        valid = position < len_ref[user]
        bias = jnp.concatenate(
            [
                jnp.broadcast_to(
                    jnp.where(valid, bias_s[head, pl.ds(user, 1), :], INVALID), (cands, block)
                )
                for head in range(heads)
            ],
            axis=0,
        )
        scores = raw * scale + bias
        top = jnp.maximum(jnp.max(scores, axis=1, keepdims=True), FLOOR)
        weights = jnp.exp2(scores - top)
        total = jnp.sum(weights, axis=1, keepdims=True)
        mixed = jnp.dot(
            weights.astype(jnp.bfloat16), v_s[slot], preferred_element_type=jnp.float32
        )
        for head in range(heads):
            held = slice(head * cands, (head + 1) * cands)
            part_s[turn, step, held, :] = mixed[held, head * size : (head + 1) * size]
        stats = column_to_row(top, 0, size) + column_to_row(total, rows, size)
        part_s[turn, step, rows : rows + 8, :] = jnp.broadcast_to(stats, (8, size))

    def exchange(turn, step):
        return pltpu.make_async_remote_copy(
            src_ref=part_s.at[turn, step],
            dst_ref=got_s.at[turn, step - 1],
            send_sem=send_sem.at[turn, step - 1],
            recv_sem=recv_sem.at[turn, step - 1],
            device_id={"seq": partner(me, step, seqs)},
            device_id_type=MESH,
        )

    def spread(turn, step):
        target = (mh + step) % slices
        return pltpu.make_async_remote_copy(
            src_ref=zpart_s.at[turn, target],
            dst_ref=zgot_s.at[turn, step - 1],
            send_sem=zsend_sem.at[turn, step - 1],
            recv_sem=zrecv_sem.at[turn, step - 1],
            device_id={"head": target},
            device_id_type=MESH,
        )

    def tell(step):
        return pltpu.make_async_remote_copy(
            src_ref=square_s,
            dst_ref=squares_s.at[step - 1],
            send_sem=tsend_sem.at[step - 1],
            recv_sem=trecv_sem.at[step - 1],
            device_id={"head": (mh + step) % slices},
            device_id_type=MESH,
        )

    def combine(turn):
        for step in range(1, seqs):
            exchange(turn, step).wait_recv()
        blocks = [part_s.at[turn, 0]] + [got_s.at[turn, step - 1] for step in range(1, seqs)]
        query = q_s[me * local + turn].astype(jnp.float32)
        new_key = nk_s[turn].astype(jnp.float32)
        new_value = nv_s[turn].astype(jnp.float32)
        product = query * new_key

        def by_head(source):
            return jnp.concatenate(
                [source[:, head * size : (head + 1) * size] for head in range(heads)], axis=0
            )

        own = jnp.sum(by_head(product), axis=1, keepdims=True) * scale
        maxima = [row_to_column(ref[rows : rows + 1, :], 0, rows) for ref in blocks]
        sums = [row_to_column(ref[rows : rows + 1, :], rows, rows) for ref in blocks]
        top = functools.reduce(jnp.maximum, maxima, own)
        own_factor = jnp.exp2(own - top)
        numer = own_factor * by_head(new_value)
        denom = own_factor
        for ref, high, amount in zip(blocks, maxima, sums):
            factor = jnp.exp2(high - top)
            numer = numer + factor * ref[:rows, :]
            denom = denom + factor * amount
        attended = numer / denom
        squares = jnp.sum(jnp.square(attended), axis=1, keepdims=True)
        square = squares[:cands]
        for head in range(1, heads):
            square = square + squares[head * cands : (head + 1) * cands]
        square_s[turn : turn + 1, :] = column_to_row(square, 0, LANES)
        if turn == local - 1:
            for step in range(1, slices):
                tell(step).start()
        wide = jnp.concatenate(
            [attended[head * cands : (head + 1) * cands] for head in range(heads)], axis=1
        )
        gate = gate_s[turn].astype(jnp.float32)
        gain = gain_s[...].reshape(1, width)
        hidden = (wide * gain * (gate / (1.0 + jnp.exp(-gate)))).astype(jnp.bfloat16)
        projected = jnp.dot(hidden, w_s[...], preferred_element_type=jnp.float32)
        for target in range(slices):
            zpart_s[turn, target] = projected[:, target * out_cols : (target + 1) * out_cols]
        for step in range(slices - 1, 0, -1):
            spread(turn, step).start()

    def finish(turn):
        total = zpart_s[turn, mh]
        for step in range(1, slices):
            spread(turn, step).wait_recv()
            total = total + zgot_s[turn, step - 1]
        out_ref[turn] = (total * factor_of(turn)).astype(out_ref.dtype)

    for turn in range(local):
        for step in range(seqs - 1, -1, -2):
            slots = [turn * seqs + seqs - 1 - step]
            if step:
                slots.append(slots[0] + 1)
            for slot in slots:
                order[slot][3].wait()
                order[slot][4].wait()
            for slot in slots:
                fetch(slot + AHEAD)
            if turn == 0 and step == seqs - 1:
                for copy in late:
                    copy.start()
            for slot in slots:
                attend(slot)
            if turn == 0 and step == seqs - 1:
                pl.semaphore_wait(barrier, seqs - 1 + slices - 1)
            for slot in slots:
                if order[slot][1]:
                    exchange(turn, order[slot][1]).start()
            if turn > 0 and step == seqs - 1:
                if turn == 1:
                    for copy in late:
                        copy.wait()
                combine(turn - 1)
    if local == 1:
        for copy in late:
            copy.wait()
    combine(local - 1)
    for step in range(1, slices):
        tell(step).wait_recv()
    square = square_s[...]
    for step in range(1, slices):
        square = square + squares_s[step - 1]

    def factor_of(turn):
        column = row_to_column(square[turn : turn + 1, :], 0, cands)
        return 1.0 / jnp.sqrt(column / (width * slices) + 1e-6)

    for turn in range(local):
        finish(turn)
    for step in range(1, slices):
        tell(step).wait_send()
    for turn in range(local):
        for step in range(1, seqs):
            exchange(turn, step).wait_send()
        for step in range(1, slices):
            spread(turn, step).wait_send()


def body(
    query,
    new_key,
    new_value,
    keys,
    values,
    lengths,
    time_bucket,
    action,
    time_bias,
    action_bias,
    gate,
    norm_gain,
    w_out,
):
    users, block, width = keys.shape
    cands = query.shape[1]
    heads = time_bias.shape[1]
    size = width // heads
    seqs = lax.axis_size("seq")
    slices = lax.axis_size("head")
    local = users // seqs
    rows = heads * cands
    lines = -(-local // 8) * 8
    out_cols = w_out.shape[1] // slices
    dims = (users, cands, block, heads, size, seqs, slices, local, out_cols)
    f32, bf16 = jnp.float32, jnp.bfloat16
    anywhere = pl.BlockSpec(memory_space=pltpu.HBM)
    return pl.pallas_call(
        functools.partial(kernel, dims),
        out_shape=jax.ShapeDtypeStruct((local, cands, out_cols), bf16),
        in_specs=[anywhere] * 13,
        out_specs=pl.BlockSpec(memory_space=pltpu.VMEM),
        scratch_shapes=[
            pltpu.SMEM((users,), jnp.int32),
            pltpu.VMEM((users, cands, width), bf16),
            pltpu.VMEM((local, cands, width), bf16),
            pltpu.VMEM((local, cands, width), bf16),
            pltpu.VMEM((users, block, width), bf16),
            pltpu.VMEM((users, block, width), bf16),
            pltpu.VMEM((users, block), jnp.int32),
            pltpu.VMEM((users, block), jnp.int32),
            pltpu.VMEM(time_bias.T.shape, f32),
            pltpu.VMEM(action_bias.T.shape, f32),
            pltpu.VMEM((local, cands, width), bf16),
            pltpu.VMEM((width,), f32),
            pltpu.VMEM(w_out.shape, bf16),
            pltpu.VMEM((heads, users, block), f32),
            pltpu.VMEM((local, seqs, rows + 8, size), f32),
            pltpu.VMEM((local, seqs - 1, rows + 8, size), f32),
            pltpu.VMEM((local, slices, cands, out_cols), f32),
            pltpu.VMEM((local, slices - 1, cands, out_cols), f32),
            pltpu.VMEM((lines, LANES), f32),
            pltpu.VMEM((slices - 1, lines, LANES), f32),
            pltpu.SemaphoreType.DMA((users,)),
            pltpu.SemaphoreType.DMA((users,)),
            pltpu.SemaphoreType.DMA((6,)),
            pltpu.SemaphoreType.DMA((5,)),
            pltpu.SemaphoreType.DMA((local, seqs - 1)),
            pltpu.SemaphoreType.DMA((local, seqs - 1)),
            pltpu.SemaphoreType.DMA((local, slices - 1)),
            pltpu.SemaphoreType.DMA((local, slices - 1)),
            pltpu.SemaphoreType.DMA((slices - 1,)),
            pltpu.SemaphoreType.DMA((slices - 1,)),
        ],
        compiler_params=pltpu.CompilerParams(
            collective_id=0, has_side_effects=True, vmem_limit_bytes=67043328
        ),
    )(
        lengths,
        query,
        new_key,
        new_value,
        keys,
        values,
        time_bucket,
        action,
        time_bias.T,
        action_bias.T,
        gate,
        norm_gain,
        w_out,
    )


def solution(mesh):
    placed = (
        P("groups", None, "head"),
        P("groups", None, "head"),
        P("groups", None, "head"),
        P("groups", "seq", "head"),
        P("groups", "seq", "head"),
        P("groups"),
        P("groups", "seq"),
        P("groups", "seq"),
        P(None, "head"),
        P(None, "head"),
        P("groups", None, "head"),
        P("head"),
        P("head", None),
    )
    return jax.shard_map(
        body,
        mesh=mesh,
        in_specs=placed,
        out_specs=P(("groups", "seq"), None, "head"),
        check_vma=False,
    )
```
